32 devices in a mesh: seq: 16 (over z, x, core), head: 2 (over y).
Axes of the slice: x: 2, y: 2, z: 4, core: 2. Of those that a mesh axis runs over, the one named last changes fastest.
Arguments:
- query: bfloat16 [8192, 1024], P('seq', 'head'), may hold values from -6 to 6
- key_rows: bfloat16 [8192, 128], P('seq'), may hold values from -6 to 6
- value_rows: bfloat16 [8192, 128], P('seq'), may hold values from -6 to 6
- output: bfloat16 [8192, 1024], P('seq', 'head'), may hold values from -1.5 to 1.5
- grad_output: bfloat16 [8192, 1024], P('seq', 'head'), may hold values from -144 to 144
- log_norm: float32 [8, 8192], P('head', 'seq'), may hold values from 0.5 to 12
- stripe: int32 [16], replicated, may hold values from 0 to 15, each once
Outputs:
- grad_query: bfloat16 [8192, 1024], P('seq', 'head')
- grad_key: bfloat16 [8192, 128], P(('seq', 'head'))
- grad_value: bfloat16 [8192, 128], P(('seq', 'head'))
The draws below stay inside these ranges and needn't reach their ends.
Inputs may be any that keep to these rules, and one draw needn't show every extreme that they name: stripe is a permutation of 0 to 15.
All inputs are finite; a program needn't handle non-finite values.
Results may differ from the reference program's by a relative error of at most 0.0051.
Values may be sent and summed in bfloat16 or wider, within the bound.
No kernel may reach another device: no remote copies, remote signals or barrier semaphores. Data moves between devices by JAX's collectives and lax.ppermute only.
A program may use at most 192 MiB of HBM per device.

```python
import jax
import jax.numpy as jnp
from jax import lax

DH = 128
QH = 8
WINDOW = 8
S_DEV = 512
LEN = 8192
N_SEQ = 16


def draw_log_norm(key, part):
    local_row = (jnp.arange(LEN) % S_DEV).astype(jnp.float32)
    counts = WINDOW * (local_row + 0.5)
    base_level = jnp.log(counts) + 0.5
    jitter = jax.random.normal(key, (QH, LEN), jnp.float32) * 0.2
    return jnp.clip(base_level[None, :] + jitter, 0.5, 12.0).astype(jnp.float32)


def shard_levels(stream_key, shape, cuts, least, top_value):
    def one(position, parts):
        steps = jax.random.uniform(jax.random.fold_in(jax.random.fold_in(stream_key, 6), position), (parts,), jnp.float32, least / len(cuts), top_value / len(cuts))
        return jnp.repeat(jnp.exp(steps), shape[position] // parts).reshape((-1,) + (1,) * (len(shape) - position - 1))

    loudness = one(*cuts[0])
    for cut in cuts[1:]:
        loudness = loudness * one(*cut)
    return loudness


def scatter_about(rng, shape, deviation, bound, split=(), held_as=jnp.bfloat16):
    entries = jax.random.normal(rng, shape, jnp.float32) * deviation
    if len(split) > 0:
        entries = shard_levels(rng, shape, split, -0.22, 0.18) * entries
    return jnp.clip(entries, min=-bound, max=bound).astype(held_as)


def setup_inputs(seed: int = 0) -> dict:
    keys = jax.random.split(jax.random.key(seed), 8)
    query = scatter_about(keys[0], (LEN, QH * DH), 1.0, 6.0, ((0, 16), (1, 2)))
    key_rows = scatter_about(keys[1], (LEN, DH), 1.0, 6.0, ((0, 16),))
    value_rows = scatter_about(keys[2], (LEN, DH), 1.0, 6.0, ((0, 16),))
    output = scatter_about(keys[3], (LEN, QH * DH), 0.25, 1.5, ((0, 16), (1, 2)))
    grad_output = scatter_about(keys[4], (LEN, QH * DH), 24.0, 144.0, ((0, 16), (1, 2)))
    log_norm = draw_log_norm(jax.random.fold_in(keys[7], 71), 0)
    stripe = jax.random.permutation(keys[6], N_SEQ).astype(jnp.int32)
    return {"query": query, "key_rows": key_rows, "value_rows": value_rows, "output": output, "grad_output": grad_output, "log_norm": log_norm, "stripe": stripe}


def block_terms(query_heads, grad_heads, lse_rows, delta_rows, key_block, value_block, diag_open):
    extent = key_block.shape[0]
    factor = key_block.shape[1] ** -0.5
    scores = jnp.einsum("shd,td->hst", query_heads, key_block) * factor
    row_ids = lax.broadcasted_iota(jnp.int32, (extent, extent), 0)
    col_ids = lax.broadcasted_iota(jnp.int32, (extent, extent), 1)
    allowed = (col_ids < row_ids) | ((col_ids == row_ids) & diag_open)
    weights = jnp.where(allowed[None], jnp.exp(scores - lse_rows[:, :, None]), jnp.float32(0.0))
    weights_low = lax.optimization_barrier(weights.astype(jnp.bfloat16)).astype(jnp.float32)
    grad_values = jnp.einsum("hst,shd->td", weights_low, grad_heads)
    grad_weights = jnp.einsum("shd,td->hst", grad_heads, value_block)
    grad_scores = (factor * weights * (grad_weights - delta_rows[:, :, None])).astype(jnp.bfloat16)
    grad_scores = lax.optimization_barrier(grad_scores).astype(jnp.float32)
    grad_query = jnp.einsum("hst,td->shd", grad_scores, key_block)
    grad_keys = jnp.einsum("hst,shd->td", grad_scores, query_heads)
    return grad_query, jnp.stack([grad_keys, grad_values])


def reference(query, key_rows, value_rows, output, grad_output, log_norm, stripe):
    query_blocks = query.reshape(N_SEQ, S_DEV, QH, DH)
    grad_blocks = grad_output.reshape(N_SEQ, S_DEV, QH, DH)
    output_blocks = output.reshape(N_SEQ, S_DEV, QH, DH)
    lse_blocks = log_norm.reshape(QH, N_SEQ, S_DEV).transpose(1, 0, 2)
    key_blocks = key_rows.reshape(N_SEQ, S_DEV, DH)
    value_blocks = value_rows.reshape(N_SEQ, S_DEV, DH)

    def one_block(grad_kv, block_index):
        query_heads = query_blocks[block_index].astype(jnp.float32)
        grad_heads = grad_blocks[block_index].astype(jnp.float32)
        delta_rows = jnp.sum(grad_heads * output_blocks[block_index].astype(jnp.float32), axis=2).T
        lse_rows = lse_blocks[block_index]
        grad_query = jnp.zeros((S_DEV, QH, DH), jnp.float32)
        for offset in range(WINDOW):
            source = ((block_index - offset) % N_SEQ).astype(jnp.int32)
            diag_open = stripe[source] <= stripe[block_index]
            key_block = key_blocks[source].astype(jnp.float32)
            value_block = value_blocks[source].astype(jnp.float32)
            query_part, kv_part = block_terms(query_heads, grad_heads, lse_rows, delta_rows, key_block, value_block, diag_open)
            grad_query = grad_query + query_part
            grad_kv = grad_kv.at[source].add(kv_part)
        return grad_kv, grad_query.astype(jnp.bfloat16)

    start_kv = jnp.zeros((N_SEQ, 2, S_DEV, DH), jnp.float32)
    grad_kv, grad_query = lax.scan(one_block, start_kv, jnp.arange(N_SEQ, dtype=jnp.int32))
    grad_key = grad_kv[:, 0].reshape(LEN, DH).astype(jnp.bfloat16)
    grad_value = grad_kv[:, 1].reshape(LEN, DH).astype(jnp.bfloat16)
    return grad_query.reshape(LEN, QH * DH), grad_key, grad_value
```

```python
import functools

import jax
import jax.numpy as jnp
from jax import lax
from jax.experimental import pallas as pl
from jax.experimental.pallas import tpu as pltpu
from jax.sharding import PartitionSpec as P

LOG2E = 1.4426950408889634
VMEM_LIMIT = 24 << 20
NT = (((1,), (1,)), ((), ()))
NN = (((1,), (0,)), ((), ()))


def dot(a, b, dims):
    return lax.dot_general(a, b, dims, preferred_element_type=jnp.float32)


def terms_kernel(plan, backs, heads, starts_dq, *refs):
    refs = iter(refs)
    stripe = next(refs)
    me = lax.axis_index("seq")
    side = lax.axis_index("head")
    odd = lax.rem(me, 2)
    n = stripe.shape[0]
    flip = me + 1 - 2 * odd
    stripes = (stripe[me], stripe[flip])
    sources = [stripe[lax.rem(me - (1 - odd) * even - odd * uneven + n, n)] for even, uneven in backs]
    kv_refs = [[next(refs)] if whole else [next(refs), next(refs)] for whole, _ in plan]
    groups = sorted({g for _, gs in plan for g in gs})
    query, grad, level = ({g: next(refs) for g in groups} for _ in range(3))
    makes_delta = plan == ((True, (0,)),)
    if makes_delta:
        output = next(refs)
        delta = None
    else:
        delta = {g: next(refs) for g in groups}
    dq_in = {g: next(refs) for g in groups if not starts_dq[g]}
    dq = {g: next(refs) for g in groups}
    send, keep = next(refs), next(refs)
    if makes_delta:
        rows_out = next(refs)
    keys, values, keys_t, dk, dv = refs
    rows, d = keys.shape[1:]
    half = rows // 2
    mine = pl.multiple_of(side * half, half)
    theirs = pl.multiple_of((1 - side) * half, half)
    for b, (whole, _) in enumerate(plan):
        if whole:
            keys[b] = kv_refs[b][0][0]
            values[b] = kv_refs[b][0][1]
        else:
            for ref, at in zip(kv_refs[b], (mine, theirs)):
                keys[b, pl.ds(at, half), :] = ref[0]
                values[b, pl.ds(at, half), :] = ref[1]
        keys_t[b] = keys[b].T
    factor = d**-0.5
    dk[...] = jnp.zeros_like(dk)
    dv[...] = jnp.zeros_like(dv)
    ahead = lax.broadcasted_iota(jnp.int32, (half, half), 0) - lax.broadcasted_iota(
        jnp.int32, (half, half), 1
    )

    def step(h, _):
        cols = pl.ds(pl.multiple_of(h * d, d), d)
        for g in groups:
            source = dq_in.get(g)
            for b, (_, gs) in enumerate(plan):
                if g not in gs:
                    continue
                opened = (sources[b] <= stripes[g]).astype(jnp.int32)
                q = query[g][:, cols]
                do = grad[g][:, cols]
                lse = level[g][pl.ds(h, 1), :] * LOG2E
                if makes_delta:
                    product = do.astype(jnp.float32) * output[:, cols].astype(jnp.float32)
                    high = product.astype(jnp.bfloat16)
                    low = (product - high.astype(jnp.float32)).astype(jnp.bfloat16)
                    ones = jnp.ones((8, d), jnp.bfloat16)
                    dl = (dot(ones, high, NT) + dot(ones, low, NT))[:1]
                    rows_out[0, pl.ds(h, 1), :] = level[g][pl.ds(h, 1), :]
                    rows_out[1, pl.ds(h, 1), :] = dl
                else:
                    dl = delta[g][pl.ds(h, 1), :]
                for t in range(2):
                    a = t * half
                    k = keys[b, a : a + half, :]
                    v = values[b, a : a + half, :]
                    scores = dot(k, q[a:], NT)
                    probs = jnp.exp2(scores * (factor * LOG2E) - lse[:, a:])
                    edge = jnp.where(ahead < opened, probs[:, :half], 0.0)
                    probs = edge if t else jnp.concatenate([edge, probs[:, half:]], axis=1)
                    grad_probs = dot(v, do[a:], NT)
                    grad_scores = (probs * (grad_probs - dl[:, a:])).astype(jnp.bfloat16)
                    dv[b, a : a + half, :] += dot(probs.astype(jnp.bfloat16), do[a:], NN)
                    dk[b, a : a + half, :] += dot(grad_scores, q[a:], NN)
                    part = dot(keys_t[b, :, a : a + half], grad_scores, NN)
                    if source is not None:
                        part = source[cols, a:] + part
                    dq[g][cols, a:] = part
                    source = dq[g]
        return 0

    lax.fori_loop(0, heads, step, 0)
    for b in range(len(plan)):
        keep[b, 0] = dk[b, pl.ds(mine, half), :] * factor
        keep[b, 1] = dv[b, pl.ds(mine, half), :]
        send[b, 0] = (dk[b, pl.ds(theirs, half), :] * factor).astype(jnp.bfloat16)
        send[b, 1] = dv[b, pl.ds(theirs, half), :].astype(jnp.bfloat16)


def terms(plan, backs, kvs, stripe, query, grad, level, delta, dq_in, output=None):
    groups = sorted({g for _, gs in plan for g in gs})
    n = len(plan)
    rows, width = query[0].shape
    d = kvs[0].shape[-1]
    heads = width // d
    starts_dq = [x is None for x in dq_in]
    carried = [dq_in[g] for g in groups if dq_in[g] is not None]
    operands = [stripe, *kvs]
    for per_group in (query, grad, level):
        operands += [per_group[g] for g in groups]
    operands += [output] if output is not None else [delta[g] for g in groups]
    at = len(operands)
    operands += carried
    aliases = {}
    for place, g in enumerate(groups):
        if dq_in[g] is not None:
            aliases[at + len(aliases)] = place
    pairs = sum(len(gs) for _, gs in plan)
    vmem = pl.BlockSpec(memory_space=pltpu.VMEM)
    halves = (n, 2, rows // 2, d)
    extra = [] if output is None else [jax.ShapeDtypeStruct((2, heads, rows), jnp.float32)]
    out = pl.pallas_call(
        functools.partial(terms_kernel, plan, backs, heads, starts_dq),
        out_shape=[jax.ShapeDtypeStruct((width, rows), jnp.float32) for _ in groups]
        + [jax.ShapeDtypeStruct(halves, jnp.bfloat16), jax.ShapeDtypeStruct(halves, jnp.float32)]
        + extra,
        in_specs=[pl.BlockSpec(memory_space=pltpu.SMEM)] + [vmem] * (len(operands) - 1),
        out_specs=[vmem] * (len(groups) + 2 + len(extra)),
        input_output_aliases=aliases,
        scratch_shapes=[
            pltpu.VMEM((n, rows, d), jnp.bfloat16),
            pltpu.VMEM((n, rows, d), jnp.bfloat16),
            pltpu.VMEM((n, d, rows), jnp.bfloat16),
            pltpu.VMEM((n, rows, d), jnp.float32),
            pltpu.VMEM((n, rows, d), jnp.float32),
        ],
        cost_estimate=pl.CostEstimate(
            flops=pairs * heads * rows * rows * d * 8,
            bytes_accessed=4 * rows * width * 2,
            transcendentals=pairs * heads * rows * rows,
        ),
        compiler_params=pltpu.CompilerParams(vmem_limit_bytes=VMEM_LIMIT),
        name="window_terms",
    )(*operands)
    dq = list(dq_in)
    for place, g in enumerate(groups):
        dq[g] = out[place]
    return dq, *out[len(groups) :]


def shards(query, key_rows, value_rows, output, grad_output, log_norm, stripe):
    rows, width = query.shape
    d = key_rows.shape[1]
    heads = width // d
    half = rows // 2
    n = lax.axis_size("seq")
    me = lax.axis_index("seq")
    side = lax.axis_index("head")
    def shift(x, by, only_odd=False):
        route = [(i, (i + by) % n) for i in range(n) if i % 2 or not only_odd]
        return lax.ppermute(x, "seq", route)

    def flip_core(x):
        return lax.ppermute(x, "seq", [(i, i ^ 1) for i in range(n)])

    def flip_head(x):
        return lax.ppermute(x, "head", [(0, 1), (1, 0)])

    kv = jnp.stack([key_rows, value_rows])
    kv_mine = lax.dynamic_slice_in_dim(kv, side * half, half, 1)
    kv_theirs = lax.dynamic_slice_in_dim(kv, (1 - side) * half, half, 1)
    near = [shift(kv_mine, 2), shift(kv_mine, 4)]
    far = [shift(kv_mine, 6), shift(kv_mine, 8, only_odd=True)]

    queries = [query, flip_core(query)]
    grads = [grad_output, flip_core(grad_output)]
    dq, own_send, own_keep, level_delta = terms(
        ((True, (0,)),),
        ((0, 0),),
        [kv],
        stripe,
        queries,
        grads,
        [log_norm],
        None,
        [None, None],
        output,
    )
    other_rows = flip_core(level_delta)
    args = (
        queries,
        grads,
        [log_norm, other_rows[0]],
        [level_delta[1], other_rows[1]],
    )

    near_flip = flip_head(jnp.stack(near))
    far_flip = flip_head(jnp.stack(far))

    dq, near_send, near_keep = terms(
        ((False, (0, 1)), (False, (0, 1))),
        ((2, 2), (4, 4)),
        [near[0], near_flip[0], near[1], near_flip[1]],
        stripe,
        *args,
        dq,
    )
    is_odd = me % 2 == 1
    last = [jnp.where(is_odd, far[1], kv_mine), jnp.where(is_odd, far_flip[1], kv_theirs)]
    dq, far_send, far_keep = terms(
        ((False, (0, 1)), (False, (1,))),
        ((6, 6), (0, 8)),
        [far[0], far_flip[0], *last],
        stripe,
        *args,
        dq,
    )

    grad_query = (dq[0] + flip_core(dq[1])) * (d**-0.5)
    grad_query = grad_query.T.astype(jnp.bfloat16)

    own = own_keep[0] + flip_head(own_send)[0].astype(jnp.float32)
    near_sum = (near_keep + flip_head(near_send).astype(jnp.float32)).astype(jnp.bfloat16)
    back = [shift(near_sum[0], -2), shift(near_sum[1], -4)]
    far_sum = far_keep + flip_head(far_send).astype(jnp.float32)
    far_low = far_sum.astype(jnp.bfloat16)
    back += [shift(far_low[0], -6), shift(far_low[1], -8, only_odd=True)]
    own = own + jnp.where(is_odd, 0.0, far_sum[1])
    for part in back:
        own = own + part.astype(jnp.float32)
    own = own.astype(jnp.bfloat16)
    return grad_query, own[0], own[1]


def solution(mesh):
    placed = (
        P("seq", "head"),
        P("seq", None),
        P("seq", None),
        P("seq", "head"),
        P("seq", "head"),
        P("head", "seq"),
        P(),
    )
    return jax.shard_map(
        shards,
        mesh=mesh,
        in_specs=placed,
        out_specs=(P("seq", "head"), P(("seq", "head"), None), P(("seq", "head"), None)),
        check_vma=False,
    )
```

```python
import functools

import jax
import jax.numpy as jnp
from jax import lax
from jax.experimental import pallas as pl
from jax.experimental.pallas import tpu as pltpu
from jax.sharding import PartitionSpec as P


LOG2E = 1.4426950408889634
VMEM_LIMIT = 24 << 20
SMEM = pl.BlockSpec(memory_space=pltpu.SMEM)
BACKS = ((0, 0), (2, 2), (4, 4), (6, 6), (0, 8))
NT = (((1,), (1,)), ((), ()))
NN = (((1,), (0,)), ((), ()))


def dot(a, b, dims):
    return lax.dot_general(a, b, dims, preferred_element_type=jnp.float32)


def terms_kernel(plan, place, heads, starts_dq, *refs):
    blocks, groups = plan
    refs = iter(refs)
    opens = next(refs)
    side = lax.axis_index("head")
    odd = lax.rem(lax.axis_index("seq"), 2)
    kv_refs = [next(refs) for _ in range(blocks)]
    query_grad, level = ({g: next(refs) for g in groups} for _ in range(2))
    dq_in = {g: next(refs) for g in groups if not starts_dq[g]}
    dq = {g: next(refs) for g in groups}
    send, keep = next(refs), next(refs)
    keys, values, keys_t, dk, dv = refs
    rows, d = keys.shape
    half = rows // 2
    mine = pl.multiple_of(side * half, half)
    theirs = pl.multiple_of((1 - side) * half, half)

    def take(ref):
        keys[...] = ref[0]
        values[...] = ref[1]

    if len(kv_refs) == 1:
        take(kv_refs[0])
    else:
        for parity, ref in enumerate(kv_refs):
            pl.when(odd == parity)(functools.partial(take, ref))
    keys_t[...] = keys[...].T
    factor = d**-0.5
    dk[...] = jnp.zeros_like(dk)
    dv[...] = jnp.zeros_like(dv)
    ahead = lax.broadcasted_iota(jnp.int32, (half, half), 0) - lax.broadcasted_iota(
        jnp.int32, (half, half), 1
    )

    opened = {g: opens[2 * place + g : 2 * place + g + 1, :] for g in groups}
    written = set()

    def query(h, g, s):
        return query_grad[g][s : s + half, h * d : h * d + d]

    def grad(h, g, s):
        return query_grad[g][s : s + half, (heads + h) * d : (heads + h) * d + d]

    def scores_of(h, g, a, s):
        scores = dot(keys[a : a + half, :], query(h, g, s), NT)
        grad_probs = dot(values[a : a + half, :], grad(h, g, s), NT)
        return scores, grad_probs

    def gradients_of(h, g, a, s, scores, grad_probs):
        cols = slice(h * d, h * d + d)
        spot = slice(s, s + half)
        probs = jnp.exp2(scores * (factor * LOG2E) - level[g][0, h : h + 1, spot] * LOG2E)
        if s == a:
            probs = jnp.where(ahead < opened[g], probs, 0.0)
        grad_scores = (probs * factor) * (grad_probs - level[g][1, h : h + 1, spot])
        grad_scores = grad_scores.astype(jnp.bfloat16)
        dv[a : a + half, :] += dot(probs.astype(jnp.bfloat16), grad(h, g, s), NN)
        dk[a : a + half, :] += dot(grad_scores, query(h, g, s), NN)
        part = dot(keys_t[:, a : a + half], grad_scores, NN)
        before = dq[g] if (h, g, s) in written else dq_in.get(g)
        dq[g][cols, spot] = part if before is None else before[cols, spot] + part
        written.add((h, g, s))

    tiles = [
        (h, g, a, s)
        for h in range(heads)
        for g in groups
        for a in (0, half)
        for s in range(a, rows, half)
    ]
    last = None
    for tile in tiles:
        ready = scores_of(*tile)
        if last is not None:
            gradients_of(*last)
        last = (*tile, *ready)
    gradients_of(*last)
    keep[0] = dk[pl.ds(mine, half), :]
    keep[1] = dv[pl.ds(mine, half), :]
    send[0] = dk[pl.ds(theirs, half), :].astype(jnp.bfloat16)
    send[1] = dv[pl.ds(theirs, half), :].astype(jnp.bfloat16)


def call(kernel, out_shape, operands, specs=None, **options):
    vmem = pl.BlockSpec(memory_space=pltpu.VMEM)
    return pl.pallas_call(
        kernel,
        out_shape=out_shape,
        in_specs=[SMEM if s else vmem for s in specs or [""] * len(operands)],
        out_specs=[vmem] * len(out_shape),
        compiler_params=pltpu.CompilerParams(vmem_limit_bytes=VMEM_LIMIT),
        **options,
    )(*operands)


def delta_kernel(d, stripe, query_grad, output, norm, rows_out, opens):
    rows_out[0] = norm[...]
    heads = norm.shape[0]
    ones = jnp.ones((8, d), jnp.bfloat16)
    for h in range(heads):
        cols = slice(h * d, h * d + d)
        grad = query_grad[:, (heads + h) * d : (heads + h) * d + d].astype(jnp.float32)
        product = grad * output[:, cols].astype(jnp.float32)
        high = product.astype(jnp.bfloat16)
        low = (product - high.astype(jnp.float32)).astype(jnp.bfloat16)
        rows_out[1, h : h + 1, :] = (dot(ones, high, NT) + dot(ones, low, NT))[:1]
    me = lax.axis_index("seq")
    odd = lax.rem(me, 2)
    n = stripe.shape[0]
    for place, (even_back, odd_back) in enumerate(BACKS):
        source = stripe[lax.rem(me - (1 - odd) * even_back - odd * odd_back + n, n)]
        for g, reader in enumerate((me, me + 1 - 2 * odd)):
            is_open = (source <= stripe[reader]).astype(jnp.int32)
            opens[2 * place + g : 2 * place + g + 1, :] = jnp.full((1, opens.shape[1]), is_open)


def query_kernel(heads, mine_ref, theirs_ref, out_ref):
    d = out_ref.shape[1] // heads
    for h in range(heads):
        cols = slice(h * d, h * d + d)
        out_ref[:, cols] = (mine_ref[cols, :] + theirs_ref[cols, :]).T.astype(out_ref.dtype)


def final_kernel(keep_ref, flip_ref, keep8_ref, flip8_ref, *refs):
    *backs, key_ref, value_ref = refs
    twice = (lax.rem(lax.axis_index("seq"), 2) == 0).astype(jnp.float32)
    for i, out in enumerate((key_ref, value_ref)):
        total = keep_ref[i] + flip_ref[i].astype(jnp.float32)
        total += twice * (keep8_ref[i] + flip8_ref[i].astype(jnp.float32))
        for back in backs:
            total += back[i].astype(jnp.float32)
        out[...] = total.astype(out.dtype)


def terms(plan, backs, kvs, opens, query_grad, level, dq_in):
    _, groups = plan
    rows = query_grad[0].shape[0]
    d = kvs[0].shape[-1]
    width = query_grad[0].shape[1] // 2
    heads = width // d
    starts_dq = [x is None for x in dq_in]
    operands = [opens, *kvs]
    for per_group in (query_grad, level):
        operands += [per_group[g] for g in groups]
    aliases = {}
    for place, g in enumerate(groups):
        if dq_in[g] is not None:
            aliases[len(operands)] = place
            operands.append(dq_in[g])
    halves = (2, rows // 2, d)
    out_shape = [jax.ShapeDtypeStruct((width, rows), jnp.float32) for _ in groups]
    out_shape += [jax.ShapeDtypeStruct(halves, jnp.bfloat16), jax.ShapeDtypeStruct(halves, jnp.float32)]
    out = call(
        functools.partial(terms_kernel, plan, BACKS.index(backs), heads, starts_dq),
        out_shape,
        operands,
        input_output_aliases=aliases,
        scratch_shapes=[
            pltpu.VMEM((rows, d), jnp.bfloat16),
            pltpu.VMEM((rows, d), jnp.bfloat16),
            pltpu.VMEM((d, rows), jnp.bfloat16),
            pltpu.VMEM((rows, d), jnp.float32),
            pltpu.VMEM((rows, d), jnp.float32),
        ],
        cost_estimate=pl.CostEstimate(
            flops=len(groups) * heads * rows * rows * d * 8,
            bytes_accessed=4 * rows * width * 2,
            transcendentals=len(groups) * heads * rows * rows,
        ),
    )
    dq = list(dq_in)
    for place, g in enumerate(groups):
        dq[g] = out[place]
    return dq, *out[len(groups) :]


def shards(query, key_rows, value_rows, output, grad_output, log_norm, stripe):
    rows, width = query.shape
    d = key_rows.shape[1]
    heads = width // d
    half = rows // 2
    n = lax.axis_size("seq")

    def shift(x, by, only_odd=False):
        route = [(i, (i + by) % n) for i in range(n) if i % 2 or not only_odd]
        return lax.ppermute(x, "seq", route)

    def flip_core(x):
        return lax.ppermute(x, "seq", [(i, i ^ 1) for i in range(n)])

    def flip_head(x):
        return lax.ppermute(x, "head", [(0, 1), (1, 0)])

    bf16 = functools.partial(jax.ShapeDtypeStruct, dtype=jnp.bfloat16)
    kv = jnp.stack([key_rows, value_rows])
    kv2 = shift(kv, 2)
    kv4 = shift(kv, 4)
    kv6 = shift(kv2, 4)
    kv8 = shift(kv4, 4, only_odd=True)
    query_grad = jnp.concatenate([query, grad_output], axis=1)
    their_query_grad = flip_core(query_grad)
    my_level, opens = call(
        functools.partial(delta_kernel, d),
        [
            jax.ShapeDtypeStruct((2, heads, rows), jnp.float32),
            jax.ShapeDtypeStruct((2 * len(BACKS), half), jnp.int32),
        ],
        [stripe, query_grad, output, log_norm],
        ["smem", "", "", ""],
    )
    args = (
        opens,
        (query_grad, their_query_grad),
        (my_level, flip_core(my_level)),
    )

    def low_sum(keep, flip):
        return (keep + flip.astype(jnp.float32)).astype(jnp.bfloat16)

    both = (0, 1)
    dq = [None, None]
    dq, send0, keep0 = terms((1, (0,)), (0, 0), [kv], *args, dq)
    dq, send2, keep2 = terms((1, both), (2, 2), [kv2], *args, dq)
    flip0, flip2 = flip_head(jnp.stack([send0, send2]))
    dq, send4, keep4 = terms((1, both), (4, 4), [kv4], *args, dq)
    flip4 = flip_head(send4)
    back2 = shift(low_sum(keep2, flip2), -2)
    dq, send6, keep6 = terms((1, both), (6, 6), [kv6], *args, dq)
    flip6 = flip_head(send6)
    back4 = shift(low_sum(keep4, flip4), -4)
    back6 = shift(low_sum(keep6, flip6), -6)
    dq, send8, keep8 = terms((2, (1,)), (0, 8), [kv, kv8], *args, dq)
    flip8 = flip_head(send8)
    their_dq = flip_core(dq[1])
    back8 = shift(low_sum(keep8, flip8), -8, only_odd=True)
    (grad_query,) = call(
        functools.partial(query_kernel, heads), [bf16((rows, width))], [dq[0], their_dq]
    )
    grad_key, grad_value = call(
        final_kernel,
        [bf16((half, d))] * 2,
        [keep0, flip0, keep8, flip8, back2, back4, back6, back8],
    )
    return grad_query, grad_key, grad_value


def solution(mesh):
    placed = (
        P("seq", "head"),
        P("seq", None),
        P("seq", None),
        P("seq", "head"),
        P("seq", "head"),
        P("head", "seq"),
        P(),
    )

    return jax.shard_map(
        shards,
        mesh=mesh,
        in_specs=placed,
        out_specs=(P("seq", "head"), P(("seq", "head"), None), P(("seq", "head"), None)),
        check_vma=False,
    )
```

```python
import functools

import jax
import jax.numpy as jnp
from jax import lax
from jax.experimental import pallas as pl
from jax.experimental.pallas import tpu as pltpu
from jax.sharding import PartitionSpec as P


LOG2E = 1.4426950408889634
VMEM_LIMIT = 24 << 20
SMEM = pl.BlockSpec(memory_space=pltpu.SMEM)
BACKS = ((0, 0), (2, 2), (4, 4), (6, 6), (0, 8))
NT = (((1,), (1,)), ((), ()))
NN = (((1,), (0,)), ((), ()))


def dot(a, b, dims):
    return lax.dot_general(a, b, dims, preferred_element_type=jnp.float32)


def terms_kernel(plan, place, heads, starts_dq, *refs):
    blocks, groups = plan
    refs = iter(refs)
    opens = next(refs)
    side = lax.axis_index("head")
    odd = lax.rem(lax.axis_index("seq"), 2)
    kv_refs = [next(refs) for _ in range(blocks)]
    query_grad, level = ({g: next(refs) for g in groups} for _ in range(2))
    dq_in = {g: next(refs) for g in groups if not starts_dq[g]}
    dq = {g: next(refs) for g in groups}
    send, keep = next(refs), next(refs)
    keys, values, keys_t, dk, dv = refs
    rows, d = keys.shape
    half = rows // 2
    mine = pl.multiple_of(side * half, half)
    theirs = pl.multiple_of((1 - side) * half, half)

    def take(ref):
        keys[...] = ref[0]
        values[...] = ref[1]

    if len(kv_refs) == 1:
        take(kv_refs[0])
    else:
        for parity, ref in enumerate(kv_refs):
            pl.when(odd == parity)(functools.partial(take, ref))
    keys_t[...] = keys[...].T
    factor = d**-0.5
    dk[...] = jnp.zeros_like(dk)
    dv[...] = jnp.zeros_like(dv)
    ahead = lax.broadcasted_iota(jnp.int32, (half, half), 0) - lax.broadcasted_iota(
        jnp.int32, (half, half), 1
    )

    opened = {g: opens[2 * place + g : 2 * place + g + 1, :] for g in groups}
    written = set()

    def query(h, g, s):
        return query_grad[g][s : s + half, h * d : h * d + d]

    def grad(h, g, s):
        return query_grad[g][s : s + half, (heads + h) * d : (heads + h) * d + d]

    def scores_of(h, g, a, s):
        scores = dot(keys[a : a + half, :], query(h, g, s), NT)
        grad_probs = dot(values[a : a + half, :], grad(h, g, s), NT)
        return scores, grad_probs

    def gradients_of(h, g, a, s, scores, grad_probs):
        cols = slice(h * d, h * d + d)
        spot = slice(s, s + half)
        probs = jnp.exp2(scores * (factor * LOG2E) - level[g][0, h : h + 1, spot] * LOG2E)
        if s == a:
            probs = jnp.where(ahead < opened[g], probs, 0.0)
        grad_scores = (probs * factor) * (grad_probs - level[g][1, h : h + 1, spot])
        grad_scores = grad_scores.astype(jnp.bfloat16)
        dv[a : a + half, :] += dot(probs.astype(jnp.bfloat16), grad(h, g, s), NN)
        dk[a : a + half, :] += dot(grad_scores, query(h, g, s), NN)
        part = dot(keys_t[:, a : a + half], grad_scores, NN)
        before = dq[g] if (h, g, s) in written else dq_in.get(g)
        dq[g][cols, spot] = part if before is None else before[cols, spot] + part
        written.add((h, g, s))

    tiles = [
        (h, g, a, s)
        for h in range(heads)
        for g in groups
        for a in (0, half)
        for s in range(a, rows, half)
    ]
    last = None
    for tile in tiles:
        ready = scores_of(*tile)
        if last is not None:
            gradients_of(*last)
        last = (*tile, *ready)
    gradients_of(*last)
    keep[0] = dk[pl.ds(mine, half), :]
    keep[1] = dv[pl.ds(mine, half), :]
    send[0] = dk[pl.ds(theirs, half), :].astype(jnp.bfloat16)
    send[1] = dv[pl.ds(theirs, half), :].astype(jnp.bfloat16)


def call(kernel, out_shape, operands, specs=None, **options):
    vmem = pl.BlockSpec(memory_space=pltpu.VMEM)
    return pl.pallas_call(
        kernel,
        out_shape=out_shape,
        in_specs=[SMEM if s else vmem for s in specs or [""] * len(operands)],
        out_specs=[vmem] * len(out_shape),
        compiler_params=pltpu.CompilerParams(vmem_limit_bytes=VMEM_LIMIT),
        **options,
    )(*operands)


def delta_kernel(d, stripe, query_grad, output, norm, rows_out, opens):
    rows_out[0] = norm[...]
    heads = norm.shape[0]
    ones = jnp.ones((8, d), jnp.bfloat16)
    for h in range(heads):
        cols = slice(h * d, h * d + d)
        grad = query_grad[:, (heads + h) * d : (heads + h) * d + d].astype(jnp.float32)
        product = grad * output[:, cols].astype(jnp.float32)
        high = product.astype(jnp.bfloat16)
        low = (product - high.astype(jnp.float32)).astype(jnp.bfloat16)
        rows_out[1, h : h + 1, :] = (dot(ones, high, NT) + dot(ones, low, NT))[:1]
    me = lax.axis_index("seq")
    odd = lax.rem(me, 2)
    n = stripe.shape[0]
    for place, (even_back, odd_back) in enumerate(BACKS):
        source = stripe[lax.rem(me - (1 - odd) * even_back - odd * odd_back + n, n)]
        for g, reader in enumerate((me, me + 1 - 2 * odd)):
            is_open = (source <= stripe[reader]).astype(jnp.int32)
            opens[2 * place + g : 2 * place + g + 1, :] = jnp.full((1, opens.shape[1]), is_open)


def query_kernel(heads, mine_ref, theirs_ref, out_ref):
    d = out_ref.shape[1] // heads
    for h in range(heads):
        cols = slice(h * d, h * d + d)
        out_ref[:, cols] = (mine_ref[cols, :] + theirs_ref[cols, :]).T.astype(out_ref.dtype)


def early_kernel(keep_ref, flip_ref, keep8_ref, flip8_ref, *refs):
    *backs, out_ref = refs
    twice = (lax.rem(lax.axis_index("seq"), 2) == 0).astype(jnp.float32)
    total = keep_ref[...] + flip_ref[...].astype(jnp.float32)
    total += twice * (keep8_ref[...] + flip8_ref[...].astype(jnp.float32))
    for back in backs:
        total += back[...].astype(jnp.float32)
    out_ref[...] = total


def final_kernel(early_ref, back_ref, key_ref, value_ref):
    for i, out in enumerate((key_ref, value_ref)):
        out[...] = (early_ref[i] + back_ref[i].astype(jnp.float32)).astype(out.dtype)


def terms(plan, backs, kvs, opens, query_grad, level, dq_in):
    _, groups = plan
    rows = query_grad[0].shape[0]
    d = kvs[0].shape[-1]
    width = query_grad[0].shape[1] // 2
    heads = width // d
    starts_dq = [x is None for x in dq_in]
    operands = [opens, *kvs]
    for per_group in (query_grad, level):
        operands += [per_group[g] for g in groups]
    aliases = {}
    for place, g in enumerate(groups):
        if dq_in[g] is not None:
            aliases[len(operands)] = place
            operands.append(dq_in[g])
    halves = (2, rows // 2, d)
    out_shape = [jax.ShapeDtypeStruct((width, rows), jnp.float32) for _ in groups]
    out_shape += [jax.ShapeDtypeStruct(halves, jnp.bfloat16), jax.ShapeDtypeStruct(halves, jnp.float32)]
    out = call(
        functools.partial(terms_kernel, plan, BACKS.index(backs), heads, starts_dq),
        out_shape,
        operands,
        input_output_aliases=aliases,
        scratch_shapes=[
            pltpu.VMEM((rows, d), jnp.bfloat16),
            pltpu.VMEM((rows, d), jnp.bfloat16),
            pltpu.VMEM((d, rows), jnp.bfloat16),
            pltpu.VMEM((rows, d), jnp.float32),
            pltpu.VMEM((rows, d), jnp.float32),
        ],
        cost_estimate=pl.CostEstimate(
            flops=len(groups) * heads * rows * rows * d * 8,
            bytes_accessed=4 * rows * width * 2,
            transcendentals=len(groups) * heads * rows * rows,
        ),
    )
    dq = list(dq_in)
    for place, g in enumerate(groups):
        dq[g] = out[place]
    return dq, *out[len(groups) :]


def shards(query, key_rows, value_rows, output, grad_output, log_norm, stripe):
    rows, width = query.shape
    d = key_rows.shape[1]
    heads = width // d
    half = rows // 2
    n = lax.axis_size("seq")

    def shift(x, by, only_odd=False):
        route = [(i, (i + by) % n) for i in range(n) if i % 2 or not only_odd]
        return lax.ppermute(x, "seq", route)

    def flip_core(x):
        return lax.ppermute(x, "seq", [(i, i ^ 1) for i in range(n)])

    def flip_head(x):
        return lax.ppermute(x, "head", [(0, 1), (1, 0)])

    bf16 = functools.partial(jax.ShapeDtypeStruct, dtype=jnp.bfloat16)
    kv = jnp.stack([key_rows, value_rows])
    kv2 = shift(kv, 2)
    kv4 = shift(kv, 4)
    kv6 = shift(kv2, 4)
    kv8 = shift(kv4, 4, only_odd=True)
    query_grad = jnp.concatenate([query, grad_output], axis=1)
    their_query_grad = flip_core(query_grad)
    my_level, opens = call(
        functools.partial(delta_kernel, d),
        [
            jax.ShapeDtypeStruct((2, heads, rows), jnp.float32),
            jax.ShapeDtypeStruct((2 * len(BACKS), half), jnp.int32),
        ],
        [stripe, query_grad, output, log_norm],
        ["smem", "", "", ""],
    )
    args = (
        opens,
        (query_grad, their_query_grad),
        (my_level, flip_core(my_level)),
    )

    def low_sum(keep, flip):
        return (keep + flip.astype(jnp.float32)).astype(jnp.bfloat16)

    both = (0, 1)
    dq = [None, None]
    dq, send0, keep0 = terms((1, (0,)), (0, 0), [kv], *args, dq)
    dq, send2, keep2 = terms((1, both), (2, 2), [kv2], *args, dq)
    flip0, flip2 = flip_head(jnp.stack([send0, send2]))
    dq, send4, keep4 = terms((1, both), (4, 4), [kv4], *args, dq)
    flip4 = flip_head(send4)
    back2 = shift(low_sum(keep2, flip2), -2)
    dq, send6, keep6 = terms((1, both), (6, 6), [kv6], *args, dq)
    flip6 = flip_head(send6)
    back4 = shift(low_sum(keep4, flip4), -4)
    back6 = shift(low_sum(keep6, flip6), -6)
    dq, send8, keep8 = terms((2, (1,)), (0, 8), [kv, kv8], *args, dq)
    flip8 = flip_head(send8)
    their_dq = flip_core(dq[1])
    back8 = shift(low_sum(keep8, flip8), -8, only_odd=True)
    (grad_query,) = call(
        functools.partial(query_kernel, heads), [bf16((rows, width))], [dq[0], their_dq]
    )
    (early,) = call(
        early_kernel,
        [jax.ShapeDtypeStruct((2, half, d), jnp.float32)],
        [keep0, flip0, keep8, flip8, back2, back4, back6],
    )
    grad_key, grad_value = call(final_kernel, [bf16((half, d))] * 2, [early, back8])
    return grad_query, grad_key, grad_value


def solution(mesh):
    placed = (
        P("seq", "head"),
        P("seq", None),
        P("seq", None),
        P("seq", "head"),
        P("seq", "head"),
        P("head", "seq"),
        P(),
    )

    return jax.shard_map(
        shards,
        mesh=mesh,
        in_specs=placed,
        out_specs=(P("seq", "head"), P(("seq", "head"), None), P(("seq", "head"), None)),
        check_vma=False,
    )
```
